32 devices in a mesh: src: 8 (over z, y), reg: 4 (over x, core).
Axes of the slice: x: 2, y: 2, z: 4, core: 2. Of those that a mesh axis runs over, the one named last changes fastest.
Arguments:
- tiles: bfloat16 [16384, 128, 128], P(('src', 'reg')), may hold values from -0.1875 to 0.1875
- rays: float32 [2048, 128], P(('src', 'reg')), may hold values from -6 to 6
- tile_rows: int32 [16384], P(('src', 'reg')), may hold values from 0 to 63, as said below
- tile_slots: int32 [16384], P(('src', 'reg')), may hold values from 0 to 63, as said below
- tile_count: int32 [32], P(('src', 'reg')), may hold values from 64 to 512, as said below
- wanted: int32 [32, 32, 2], P(('src', 'reg')), may hold values from 0 to 255
Outputs:
- solution: float32 [8192, 128], P(('src', 'reg'))
- right_vector: float32 [8192, 128], P(('src', 'reg'))
The draws below stay inside these ranges and needn't reach their ends.
Inputs may be any that keep to these rules, and one draw needn't show every extreme that they name: `tile_rows`: non-decreasing along each device's 512 tiles. `tile_slots`: the first 64 tiles of each device name every slot once. `tile_count`: some device has all 512 tiles live.
All inputs are finite; a program needn't handle non-finite values.
Results may differ from the reference program's by a relative error of at most 0.024.
Values may be sent and summed in bfloat16 or wider, within the bound.
A program may use at most 128 MiB of HBM per device.

```python
import jax
import jax.numpy as jnp
from jax import lax

TILE = 128
BLK_DEV = 256
RB_DEV = 64
TILE_SLOTS_EACH = 512
CAP = 2
ITERS = 3
NRAYBLK = 2048
NTILE = 16384
CELL_BLOCK_SLOTS = 64
DEVICES = 32


def draw_tile_rows(key, part):
    device_list = NTILE // TILE_SLOTS_EACH
    values = jax.random.randint(key, (device_list, TILE_SLOTS_EACH), 0, RB_DEV)
    return jnp.sort(values, axis=1).reshape(-1).astype(jnp.int32)


def draw_tile_slots(key, part):
    device_list = NTILE // TILE_SLOTS_EACH
    leading_part, trailing_part = jax.random.split(jax.random.fold_in(key, 7))
    random_keys = jax.random.split(leading_part, device_list)
    running_offsets = jax.vmap(lambda iteration_index: jax.random.permutation(iteration_index, CELL_BLOCK_SLOTS))(random_keys).astype(jnp.int32)
    remaining_part = jax.random.randint(trailing_part, (device_list, TILE_SLOTS_EACH - CELL_BLOCK_SLOTS), 0, CELL_BLOCK_SLOTS).astype(jnp.int32)
    return jnp.concatenate([running_offsets, remaining_part], axis=1).reshape(-1).astype(jnp.int32)


def draw_tile_count(key, part):
    leading_part, trailing_part = jax.random.split(key)
    device_list = NTILE // TILE_SLOTS_EACH
    entry_counts = jax.random.randint(leading_part, (device_list,), CELL_BLOCK_SLOTS, TILE_SLOTS_EACH + 1)
    filled = jax.random.randint(trailing_part, (), 0, device_list)
    return entry_counts.at[filled].set(TILE_SLOTS_EACH).astype(jnp.int32)


def touch_ends(entries, stream_key, low, top_value):
    spot = [jax.random.randint(jax.random.fold_in(stream_key, axis), (), 0, length) for axis, length in enumerate(entries.shape)]
    widest = entries.shape.index(max(entries.shape))
    beside = spot[:widest] + [(spot[widest] + 1) % entries.shape[widest]] + spot[widest + 1:]
    return entries.at[tuple(spot)].set(low).at[tuple(beside)].set(top_value)


def steps_of(stream_key, extent, pieces, smallest, high):
    gain = 1.0
    for position, shards_of in pieces:
        draws = jax.random.uniform(jax.random.fold_in(jax.random.fold_in(stream_key, 6), position), (shards_of,), jnp.float32, smallest / len(pieces), high / len(pieces))
        gain = gain * jnp.repeat(jnp.exp(draws), extent[position] // shards_of).reshape((-1,) + (1,) * (len(extent) - 1 - position))
    return gain


def scatter_about(own_key, extent, spread, limit, pieces=(), kind=jnp.bfloat16):
    values = spread * jax.random.normal(own_key, extent, jnp.float32)
    if pieces:
        values = values * steps_of(own_key, extent, pieces, -0.22, 0.18)
    return jnp.clip(values, -limit, limit).astype(kind)


def setup_inputs(seed: int = 0) -> dict:
    arg_keys = jax.random.split(jax.random.key(seed), 7)
    tiles = scatter_about(arg_keys[0], (NTILE, TILE, TILE), (TILE_SLOTS_EACH * TILE // RB_DEV) ** -0.5, 0.1875, ((0, 32),))
    rays = scatter_about(arg_keys[1], (NRAYBLK, TILE), 1.0, 6.0, ((0, 32),), jnp.float32)
    tile_rows = draw_tile_rows(jax.random.fold_in(arg_keys[6], 71), 0)
    tile_slots = draw_tile_slots(jax.random.fold_in(arg_keys[6], 71), 0)
    tile_count = draw_tile_count(jax.random.fold_in(arg_keys[6], 71), 0)
    wanted = touch_ends(jax.random.randint(arg_keys[5], (DEVICES, DEVICES, CAP), 0, BLK_DEV), jax.random.fold_in(arg_keys[5], 1), 0, BLK_DEV - 1).astype(jnp.int32)
    return {"tiles": tiles, "rays": rays, "tile_rows": tile_rows, "tile_slots": tile_slots, "tile_count": tile_count, "wanted": wanted}


damping = 0.5

def column_blocks(tile_slots, wanted, blocks_dev):
    device_list = wanted.shape[0]
    cap = wanted.shape[2]
    slots = tile_slots.reshape(device_list, -1)
    owner = slots // cap
    within = slots % cap
    asking = jnp.arange(device_list, dtype=jnp.int32)[:, None]
    local = wanted[owner, asking, within]
    return (owner * blocks_dev + local).astype(jnp.int32)

def forward(tiles4, vec_bf, columns, rows, live, row_blocks):

    def one(args):
        tile_set, cols, row_ids, mask = args
        picked = vec_bf[cols].astype(jnp.float32)
        prod = jnp.einsum('tij,tj->ti', tile_set.astype(jnp.float32), picked, precision=lax.Precision.HIGHEST)
        prod = prod * mask[:, None]
        return jax.ops.segment_sum(prod, row_ids, num_segments=row_blocks)
    result = lax.map(one, (tiles4, columns, rows, live))
    return result.reshape(-1, tiles4.shape[-1])

def adjoint(tiles4, ray_bf, columns, rows, live, total_blocks):
    device_list = tiles4.shape[0]
    width = tiles4.shape[-1]
    ray_dev = ray_bf.reshape(device_list, -1, width)

    def step(total, args):
        tile_set, cols, row_ids, mask, ray_set = args
        picked = ray_set[row_ids].astype(jnp.float32)
        contrib = jnp.einsum('tij,ti->tj', tile_set.astype(jnp.float32), picked, precision=lax.Precision.HIGHEST)
        contrib = contrib * mask[:, None]
        return (total.at[cols].add(contrib), None)
    start = jnp.zeros((total_blocks, width), jnp.float32)
    total, _ = lax.scan(step, start, (tiles4, columns, rows, live, ray_dev))
    return total

def reference(tiles, rays, tile_rows, tile_slots, tile_count, wanted):
    device_list = wanted.shape[0]
    width = tiles.shape[-1]
    total_blocks = BLK_DEV * device_list
    tiles4 = tiles.reshape(device_list, -1, width, width)
    per_dev = tiles4.shape[1]
    rows = tile_rows.reshape(device_list, per_dev)
    row_blocks = rays.shape[0] // device_list
    live = (jnp.arange(per_dev, dtype=jnp.int32)[None, :] < tile_count[:, None]).astype(jnp.float32)
    columns = column_blocks(tile_slots, wanted, BLK_DEV)
    u = jnp.zeros_like(rays)
    v = jnp.zeros((total_blocks, width), jnp.float32)
    solution = jnp.zeros((total_blocks, width), jnp.float32)
    w = jnp.zeros((total_blocks, width), jnp.float32)
    uraw = rays
    vraw = v
    alpha = jnp.float32(1.0)
    phibar = jnp.float32(0.0)
    rhobar = jnp.float32(0.0)
    for step in range(ITERS + 1):
        if step > 0:
            uraw = forward(tiles4, vraw.astype(jnp.bfloat16), columns, rows, live, row_blocks) / alpha - alpha * u
        beta = jnp.sqrt(jnp.sum(uraw * uraw))
        u = uraw / beta
        grad = adjoint(tiles4, uraw.astype(jnp.bfloat16), columns, rows, live, total_blocks)
        vraw = grad / beta - beta * v
        alpha_new = jnp.sqrt(jnp.sum(vraw * vraw))
        v_new = vraw / alpha_new
        if step == 0:
            w = v_new
            phibar = beta
            rhobar = alpha_new
        else:
            rhobar1 = jnp.sqrt(rhobar * rhobar + damping * damping)
            phibar = rhobar / rhobar1 * phibar
            rho = jnp.sqrt(rhobar1 * rhobar1 + beta * beta)
            cosine = rhobar1 / rho
            sine = beta / rho
            theta = sine * alpha_new
            rhobar = -cosine * alpha_new
            phi = cosine * phibar
            phibar = sine * phibar
            solution = solution + phi / rho * w
            w = v_new - theta / rho * w
        v = v_new
        alpha = alpha_new
    scale = jnp.sqrt(jnp.float32(total_blocks * width))
    return (solution, v * scale)
```

```python
import functools

import jax
import jax.numpy as jnp
from jax import lax
from jax.experimental import pallas as pl
from jax.experimental.pallas import tpu as pltpu
from jax.sharding import PartitionSpec as P

BLK_DEV = 256
ITERS = 3
damping = 0.5

GROUP = 16
HALF = GROUP // 2
F32 = jnp.float32
BF16 = jnp.bfloat16
MESH = pl.DeviceIdType.MESH


def one_hot_dot(hot, x, parts=2):
    total = None
    for part in range(parts):
        piece = x.astype(BF16)
        prod = jnp.dot(hot, piece, preferred_element_type=F32)
        total = prod if total is None else total + prod
        if part < parts - 1:
            x = x - piece.astype(F32)
    return total


def kernel(
    n, regs, stride, cap, chunks,
    tiles_hbm, rays_ref, rows_row, rows_col, slots_row, slots_col, req_row, req_col,
    sol_ref, right_ref,
    tiles_ref, left_ref, mid_ref, slot_hot, slot_hot_t, ray_hot, ray_hot_t, same_ref,
    send_ref, recv_ref, tile_sem, send_sem, recv_sem,
):
    src = lax.axis_index("src")
    reg = lax.axis_index("reg")
    me = src * regs + reg
    count = tiles_ref.shape[0]
    width = tiles_ref.shape[2]
    per_chunk = count // chunks
    groups = count // GROUP
    rows = n * stride
    row_blocks = rays_ref.shape[0]

    def tile_copy(c):
        part = pl.ds(c * per_chunk, per_chunk)
        return pltpu.make_async_copy(tiles_hbm.at[part], tiles_ref.at[part], tile_sem.at[c])

    for c in range(chunks):
        tile_copy(c).start()

    barrier = pltpu.get_barrier_semaphore()

    @pl.loop(1, n)
    def _(k):
        d = lax.rem(me + k, n)
        pl.semaphore_signal(
            barrier, inc=1, device_id=(d // regs, lax.rem(d, regs)), device_id_type=MESH
        )

    def hot(a, b):
        return jnp.where(a == b, 1.0, 0.0).astype(BF16)

    iota = functools.partial(lax.broadcasted_iota, jnp.int32)
    slot_hot[...] = hot(iota((rows, count), 0), slots_row[...])
    slot_hot_t[...] = hot(iota((count, rows), 1), slots_col[...])
    ray_hot[...] = hot(iota((row_blocks, count), 0), rows_row[...])
    ray_hot_t[...] = hot(iota((count, row_blocks), 1), rows_col[...])
    same = (req_col[...] == req_row[...]) & (req_col[...] >= 0)
    same_ref[...] = jnp.where(same, 1.0, 0.0).astype(BF16)
    lower = jnp.where(same & (iota((rows, rows), 1) < iota((rows, rows), 0)), 1.0, 0.0)
    upper = jnp.where(same & (iota((rows, rows), 0) < iota((rows, rows), 1)), 1.0, 0.0)
    first_col = jnp.where(jnp.sum(lower, axis=1, keepdims=True) == 0.0, 1.0, 0.0)
    first_row = jnp.where(jnp.sum(upper, axis=0, keepdims=True) == 0.0, 1.0, 0.0)
    place = lax.rem(iota((rows, width), 0), stride)
    is_sum = place == cap

    spot = lax.rem(iota((GROUP, width), 0), HALF)
    masks = [jnp.where(spot == b, 1.0, 0.0).astype(BF16) for b in range(HALF)]

    def spread(g):
        base = pl.multiple_of(g * GROUP, GROUP)
        left = left_ref[pl.ds(base, GROUP), :]
        return base, jnp.concatenate([left * m for m in masks], axis=1)

    def keep(base, out):
        mid_ref[pl.ds(base, HALF), :] = out[:HALF, :width]
        mid_ref[pl.ds(pl.multiple_of(base + HALF, HALF), HALF), :] = out[HALF:, width:]

    def adjoint_group(g):
        base, left = spread(g)
        a = tiles_ref[pl.ds(base, HALF)].reshape(HALF * width, width)
        b = tiles_ref[pl.ds(base + HALF, HALF)].reshape(HALF * width, width)
        right = jnp.concatenate([a, b], axis=1)
        keep(base, jnp.dot(left, right, preferred_element_type=F32))

    def forward_group(g):
        base, left = spread(g)
        halves = [
            jnp.concatenate([tiles_ref[base + h * HALF + b] for b in range(HALF)], axis=1)
            for h in range(2)
        ]
        right = jnp.concatenate(halves, axis=0)
        keep(
            base,
            lax.dot_general(
                left, right, (((1,), (1,)), ((), ())), preferred_element_type=F32
            ),
        )

    def exchange(phase, value, during=None):
        send_ref[phase] = value.reshape(n, stride, width)

        @pl.loop(1, n)
        def _(k):
            d = lax.rem(me + k, n)
            pltpu.make_async_remote_copy(
                src_ref=send_ref.at[phase, d],
                dst_ref=recv_ref.at[phase, me],
                send_sem=send_sem.at[phase],
                recv_sem=recv_sem.at[phase],
                device_id=(d // regs, lax.rem(d, regs)),
                device_id_type=MESH,
            ).start()

        recv_ref[phase, me] = send_ref[phase, me]
        others = pl.ds(0, n - 1)
        pltpu.make_async_copy(
            recv_ref.at[phase, others], recv_ref.at[phase, others], recv_sem.at[phase]
        ).wait()
        got = recv_ref[phase].reshape(rows, width)
        return got, jnp.sum(jnp.where(is_sum, got, 0.0), keepdims=True)

    uraw = rays_ref[...]
    u = None
    v = w = update = jnp.zeros((rows, width), F32)
    alpha = phibar = rhobar = None
    fetched = None
    for step in range(ITERS + 1):
        if step > 0:
            left_ref[...] = jnp.dot(
                slot_hot_t[...], fetched.astype(BF16), preferred_element_type=F32
            ).astype(BF16)

            @pl.loop(0, groups, unroll=2)
            def _(g):
                forward_group(g)

            uraw = one_hot_dot(ray_hot[...], mid_ref[...]) / alpha - alpha * u
        left_ref[...] = jnp.dot(
            ray_hot_t[...], uraw.astype(BF16), preferred_element_type=F32
        ).astype(BF16)
        if step == 0:
            per = groups // chunks

            @pl.loop(0, chunks)
            def _(c):
                tile_copy(c).wait()
                for i in range(per):
                    adjoint_group(c * per + i)
        else:

            @pl.loop(0, groups, unroll=2)
            def _(g):
                adjoint_group(g)

        sums = one_hot_dot(slot_hot[...], mid_ref[...])
        squares = jnp.sum(uraw * uraw, axis=0, keepdims=True)
        if step == 0:
            pl.semaphore_wait(barrier, n - 1)
        got, uu = exchange(2 * step, jnp.where(is_sum, squares, sums))
        beta = jnp.sqrt(uu)
        u = uraw / beta
        vraw = one_hot_dot(same_ref[...], got) / beta
        if step > 0:
            vraw = vraw - beta * v
        squares = jnp.sum(vraw * vraw * first_col, axis=0, keepdims=True)
        fetched, vv = exchange(2 * step + 1, jnp.where(is_sum, squares, vraw))
        alpha = jnp.sqrt(vv)
        v = jnp.where(place < cap, vraw, 0.0) / alpha
        if step == 0:
            w = v
            phibar = beta
            rhobar = alpha
        else:
            rhobar1 = jnp.sqrt(rhobar * rhobar + damping * damping)
            phibar = rhobar / rhobar1 * phibar
            rho = jnp.sqrt(rhobar1 * rhobar1 + beta * beta)
            cosine = rhobar1 / rho
            sine = beta / rho
            theta = sine * alpha
            rhobar = -cosine * alpha
            phi = cosine * phibar
            phibar = sine * phibar
            update = update + phi / rho * w
            w = v - theta / rho * w
    blocks = sol_ref.shape[0]
    out_hot = jnp.where(
        iota((blocks, rows), 0) == req_row[...], first_row, 0.0
    ).astype(BF16)
    scale = float(blocks * width * n) ** 0.5
    sol_ref[...] = one_hot_dot(out_hot, update, 3)
    right_ref[...] = one_hot_dot(out_hot, v * scale, 3)
    for phase in range(2 * (ITERS + 1)):
        others = pl.ds(0, n - 1)
        pltpu.make_async_copy(
            send_ref.at[phase, others], send_ref.at[phase, others], send_sem.at[phase]
        ).wait()


def per_device(n, regs, tiles, rays, tile_rows, tile_slots, tile_count, wanted):
    count, width = tiles.shape[0], tiles.shape[2]
    cap = wanted.shape[2]
    stride = 4
    while stride < cap + 1:
        stride *= 2
    rows = n * stride
    chunks = 16
    phases = 2 * (ITERS + 1)
    row_blocks = rays.shape[0]
    live = jnp.arange(count, dtype=jnp.int32) < tile_count[0]
    ray_ids = jnp.where(live, tile_rows, -1)
    slot_ids = jnp.where(live, tile_slots // cap * stride + tile_slots % cap, -1)
    requests = jnp.pad(wanted[0], ((0, 0), (0, stride - cap)), constant_values=-1).reshape(-1)
    vmem = pl.BlockSpec(memory_space=pltpu.VMEM)
    out = jax.ShapeDtypeStruct((BLK_DEV, width), F32)
    return pl.pallas_call(
        functools.partial(kernel, n, regs, stride, cap, chunks),
        out_shape=(out, out),
        in_specs=[pl.BlockSpec(memory_space=pl.ANY)] + [vmem] * 7,
        out_specs=(vmem, vmem),
        scratch_shapes=[
            pltpu.VMEM(tiles.shape, BF16),
            pltpu.VMEM((count, width), BF16),
            pltpu.VMEM((count, width), F32),
            pltpu.VMEM((rows, count), BF16),
            pltpu.VMEM((count, rows), BF16),
            pltpu.VMEM((row_blocks, count), BF16),
            pltpu.VMEM((count, row_blocks), BF16),
            pltpu.VMEM((rows, rows), BF16),
            pltpu.VMEM((phases, n, stride, width), F32),
            pltpu.VMEM((phases, n, stride, width), F32),
            pltpu.SemaphoreType.DMA((chunks,)),
            pltpu.SemaphoreType.DMA((phases,)),
            pltpu.SemaphoreType.DMA((phases,)),
        ],
        compiler_params=pltpu.CompilerParams(
            collective_id=0, has_side_effects=True, vmem_limit_bytes=56 * 1024 * 1024
        ),
    )(
        tiles,
        rays,
        ray_ids[None, :],
        ray_ids[:, None],
        slot_ids[None, :],
        slot_ids[:, None],
        requests[None, :],
        requests[:, None],
    )


def solution(mesh):
    both = ("src", "reg")
    in_specs = (
        P(both, None, None),
        P(both, None),
        P(both),
        P(both),
        P(both),
        P(both, None, None),
    )
    out_specs = (P(both, None), P(both, None))
    n = mesh.shape["src"] * mesh.shape["reg"]
    return jax.shard_map(
        functools.partial(per_device, n, mesh.shape["reg"]),
        mesh=mesh,
        in_specs=in_specs,
        out_specs=out_specs,
        check_vma=False,
    )
```

```python
import functools

import jax
import jax.numpy as jnp
from jax import lax
from jax.experimental import pallas as pl
from jax.experimental.pallas import tpu as pltpu
from jax.sharding import PartitionSpec as P

BLK_DEV = 256
ITERS = 3
damping = 0.5

GROUP = 16
HALF = GROUP // 2
TURN = 4
F32 = jnp.float32
BF16 = jnp.bfloat16
MESH = pl.DeviceIdType.MESH


def one_hot_dot(hot, x, parts=2):
    total = None
    for part in range(parts):
        piece = x.astype(BF16)
        prod = jnp.dot(hot, piece, preferred_element_type=F32)
        total = prod if total is None else total + prod
        if part < parts - 1:
            x = x - piece.astype(F32)
    return total


def kernel(
    n, regs, stride, cap, chunks,
    count_ref, tiles_hbm, rays_ref, rows_ref, slots_ref, wanted_ref,
    sol_ref, right_ref,
    tiles_ref, turned_ref, left_ref, mid_ref, slot_hot, slot_hot_t, ray_hot, ray_hot_t, same_ref,
    send_ref, recv_ref, tile_sem, send_sem, recv_sem,
):
    src = lax.axis_index("src")
    reg = lax.axis_index("reg")
    me = src * regs + reg
    count = tiles_ref.shape[0]
    width = tiles_ref.shape[2]
    per_chunk = count // chunks
    groups = count // GROUP
    rows = n * stride
    row_blocks = rays_ref.shape[0]

    def tile_copy(c):
        part = pl.ds(c * per_chunk, per_chunk)
        return pltpu.make_async_copy(tiles_hbm.at[part], tiles_ref.at[part], tile_sem.at[c])

    for c in range(chunks):
        tile_copy(c).start()

    barrier = pltpu.get_barrier_semaphore()

    @pl.loop(1, n)
    def _(k):
        d = lax.rem(me + k, n)
        pl.semaphore_signal(
            barrier, inc=1, device_id=(d // regs, lax.rem(d, regs)), device_id_type=MESH
        )

    def hot(a, b):
        return jnp.where(a == b, 1.0, 0.0).astype(BF16)

    iota = functools.partial(lax.broadcasted_iota, jnp.int32)
    live = iota((1, count), 1) < count_ref[0]
    slots = slots_ref[...]
    slots = jnp.where(live, slots // cap * stride + lax.rem(slots, cap), -1)
    one_slot = hot(iota((rows, count), 0), slots)
    one_ray = hot(iota((row_blocks, count), 0), jnp.where(live, rows_ref[...], -1))
    slot_hot[...] = one_slot
    slot_hot_t[...] = one_slot.T
    ray_hot[...] = one_ray
    ray_hot_t[...] = one_ray.T
    wanted = wanted_ref[...].astype(F32)
    row_place = lax.rem(iota((1, rows), 1), stride)
    col_place = lax.rem(iota((rows, 1), 0), stride)
    peers_t = jnp.where(iota((n, rows), 0) == iota((n, rows), 1) // stride, 1.0, 0.0)
    peers = jnp.where(iota((rows, n), 1) == iota((rows, n), 0) // stride, 1.0, 0.0)
    req_row = jnp.where(row_place < cap, 0.0, -1.0)
    req_col = jnp.where(col_place < cap, 0.0, -1.0)
    for k in range(cap):
        asked = wanted[k : k + 1, :]
        req_col += jnp.where(col_place == k, jnp.sum(peers * asked, axis=1, keepdims=True), 0.0)
        picked = jnp.dot(
            jnp.broadcast_to(asked, (8, n)), peers_t, preferred_element_type=F32,
            precision=lax.Precision.HIGHEST,
        )[:1]
        req_row += jnp.where(row_place == k, picked, 0.0)
    same = (req_col == req_row) & (req_col >= 0.0)
    same_ref[...] = jnp.where(same, 1.0, 0.0).astype(BF16)
    lower = jnp.where(same & (iota((rows, rows), 1) < iota((rows, rows), 0)), 1.0, 0.0)
    upper = jnp.where(same & (iota((rows, rows), 0) < iota((rows, rows), 1)), 1.0, 0.0)
    first_col = jnp.where(jnp.sum(lower, axis=1, keepdims=True) == 0.0, 1.0, 0.0)
    first_row = jnp.where(jnp.sum(upper, axis=0, keepdims=True) == 0.0, 1.0, 0.0)
    place = lax.rem(iota((rows, width), 0), stride)
    is_sum = place == cap

    spot = lax.rem(iota((GROUP, width), 0), HALF)
    masks = [jnp.where(spot == b, 1.0, 0.0).astype(BF16) for b in range(HALF)]

    def spread(g):
        base = pl.multiple_of(g * GROUP, GROUP)
        left = left_ref[pl.ds(base, GROUP), :]
        return base, jnp.concatenate([left * m for m in masks], axis=1)

    def keep(base, out):
        mid_ref[pl.ds(base, HALF), :] = out[:HALF, :width]
        mid_ref[pl.ds(pl.multiple_of(base + HALF, HALF), HALF), :] = out[HALF:, width:]

    def group(source, g):
        base, left = spread(g)
        a = source[pl.ds(base, HALF)].reshape(HALF * width, width)
        b = source[pl.ds(base + HALF, HALF)].reshape(HALF * width, width)
        right = jnp.concatenate([a, b], axis=1)
        keep(base, jnp.dot(left, right, preferred_element_type=F32))

    upper_half = me >= n // 2
    skip = jnp.where(upper_half, me, n - 1 - me)

    def exchange(phase, value, during=None):
        send_ref[phase] = value.reshape(n, stride, width)

        @pl.loop(0, n - 1)
        def _(j):
            j = j + jnp.where(j >= skip, 1, 0)
            d = jnp.where(upper_half, j, n - 1 - j)
            pltpu.make_async_remote_copy(
                src_ref=send_ref.at[phase, d],
                dst_ref=recv_ref.at[phase, me],
                send_sem=send_sem.at[phase],
                recv_sem=recv_sem.at[phase],
                device_id=(d // regs, lax.rem(d, regs)),
                device_id_type=MESH,
            ).start()

        recv_ref[phase, me] = send_ref[phase, me]
        others = pl.ds(0, n - 1)
        pltpu.make_async_copy(
            recv_ref.at[phase, others], recv_ref.at[phase, others], recv_sem.at[phase]
        ).wait()
        got = recv_ref[phase].reshape(rows, width)
        return got, jnp.sum(jnp.where(is_sum, got, 0.0), keepdims=True)

    uraw = rays_ref[...]
    u = None
    v = w = update = jnp.zeros((rows, width), F32)
    alpha = phibar = rhobar = None
    fetched = None
    for step in range(ITERS + 1):
        if step > 0:
            left_ref[...] = jnp.dot(
                slot_hot_t[...], fetched.astype(BF16), preferred_element_type=F32
            ).astype(BF16)

            @pl.loop(0, groups, unroll=2)
            def _(g):
                group(turned_ref, g)

            uraw = one_hot_dot(ray_hot[...], mid_ref[...]) / alpha - alpha * u
        left_ref[...] = jnp.dot(
            ray_hot_t[...], uraw.astype(BF16), preferred_element_type=F32
        ).astype(BF16)
        if step == 0:
            per = groups // chunks

            @pl.loop(0, chunks)
            def _(c):
                tile_copy(c).wait()
                for i in range(per):
                    group(tiles_ref, c * per + i)

                @pl.loop(0, per_chunk, unroll=TURN)
                def _(i):
                    turned_ref[c * per_chunk + i] = tiles_ref[c * per_chunk + i].T
        else:

            @pl.loop(0, groups, unroll=2)
            def _(g):
                group(tiles_ref, g)

        sums = one_hot_dot(slot_hot[...], mid_ref[...])
        squares = jnp.sum(uraw * uraw, axis=0, keepdims=True)
        if step == 0:
            pl.semaphore_wait(barrier, n - 1)
        got, uu = exchange(2 * step, jnp.where(is_sum, squares, sums))
        beta = jnp.sqrt(uu)
        u = uraw / beta
        vraw = one_hot_dot(same_ref[...], got) / beta
        if step > 0:
            vraw = vraw - beta * v
        squares = jnp.sum(vraw * vraw * first_col, axis=0, keepdims=True)
        fetched, vv = exchange(2 * step + 1, jnp.where(is_sum, squares, vraw))
        alpha = jnp.sqrt(vv)
        v = jnp.where(place < cap, vraw, 0.0) / alpha
        if step == 0:
            w = v
            phibar = beta
            rhobar = alpha
        else:
            rhobar1 = jnp.sqrt(rhobar * rhobar + damping * damping)
            phibar = rhobar / rhobar1 * phibar
            rho = jnp.sqrt(rhobar1 * rhobar1 + beta * beta)
            cosine = rhobar1 / rho
            sine = beta / rho
            theta = sine * alpha
            rhobar = -cosine * alpha
            phi = cosine * phibar
            phibar = sine * phibar
            update = update + phi / rho * w
            w = v - theta / rho * w
    blocks = sol_ref.shape[0]
    out_hot = jnp.where(
        iota((blocks, rows), 0).astype(F32) == req_row, first_row, 0.0
    ).astype(BF16)
    scale = float(blocks * width * n) ** 0.5
    sol_ref[...] = one_hot_dot(out_hot, update, 3)
    right_ref[...] = one_hot_dot(out_hot, v * scale, 3)
    for phase in range(2 * (ITERS + 1)):
        others = pl.ds(0, n - 1)
        pltpu.make_async_copy(
            send_ref.at[phase, others], send_ref.at[phase, others], send_sem.at[phase]
        ).wait()


def per_device(n, regs, tiles, rays, tile_rows, tile_slots, tile_count, wanted):
    count, width = tiles.shape[0], tiles.shape[2]
    cap = wanted.shape[2]
    stride = 4
    while stride < cap + 1:
        stride *= 2
    rows = n * stride
    chunks = 16
    phases = 2 * (ITERS + 1)
    row_blocks = rays.shape[0]
    vmem = pl.BlockSpec(memory_space=pltpu.VMEM)
    out = jax.ShapeDtypeStruct((BLK_DEV, width), F32)
    return pl.pallas_call(
        functools.partial(kernel, n, regs, stride, cap, chunks),
        out_shape=(out, out),
        in_specs=[
            pl.BlockSpec(memory_space=pltpu.SMEM),
            pl.BlockSpec(memory_space=pl.ANY),
        ]
        + [vmem] * 4,
        out_specs=(vmem, vmem),
        scratch_shapes=[
            pltpu.VMEM(tiles.shape, BF16),
            pltpu.VMEM(tiles.shape, BF16),
            pltpu.VMEM((count, width), BF16),
            pltpu.VMEM((count, width), F32),
            pltpu.VMEM((rows, count), BF16),
            pltpu.VMEM((count, rows), BF16),
            pltpu.VMEM((row_blocks, count), BF16),
            pltpu.VMEM((count, row_blocks), BF16),
            pltpu.VMEM((rows, rows), BF16),
            pltpu.VMEM((phases, n, stride, width), F32),
            pltpu.VMEM((phases, n, stride, width), F32),
            pltpu.SemaphoreType.DMA((chunks,)),
            pltpu.SemaphoreType.DMA((phases,)),
            pltpu.SemaphoreType.DMA((phases,)),
        ],
        compiler_params=pltpu.CompilerParams(
            collective_id=0, has_side_effects=True, vmem_limit_bytes=56 * 1024 * 1024
        ),
    )(
        tile_count,
        tiles,
        rays,
        tile_rows[None, :],
        tile_slots[None, :],
        wanted[0].T,
    )


def solution(mesh):
    both = ("src", "reg")
    in_specs = (
        P(both, None, None),
        P(both, None),
        P(both),
        P(both),
        P(both),
        P(both, None, None),
    )
    out_specs = (P(both, None), P(both, None))
    n = mesh.shape["src"] * mesh.shape["reg"]
    return jax.shard_map(
        functools.partial(per_device, n, mesh.shape["reg"]),
        mesh=mesh,
        in_specs=in_specs,
        out_specs=out_specs,
        check_vma=False,
    )
```

```python
import functools

import jax
import jax.numpy as jnp
from jax import lax
from jax.experimental import pallas as pl
from jax.experimental.pallas import tpu as pltpu
from jax.sharding import PartitionSpec as P

BLK_DEV = 256
ITERS = 3
damping = 0.5

GROUP = 16
HALF = GROUP // 2
F32 = jnp.float32
BF16 = jnp.bfloat16
MESH = pl.DeviceIdType.MESH


def one_hot_dot(hot, x, parts=2):
    total = None
    for part in range(parts):
        piece = x.astype(BF16)
        prod = jnp.dot(hot, piece, preferred_element_type=F32)
        total = prod if total is None else total + prod
        if part < parts - 1:
            x = x - piece.astype(F32)
    return total


def kernel(
    n, regs, stride, cap, chunks,
    count_ref, tiles_hbm, rays_ref, rows_ref, slots_ref, wanted_ref,
    sol_ref, right_ref,
    tiles_ref, turned_ref, left_ref, mid_ref, slot_hot, slot_hot_t, ray_hot, ray_hot_t, same_ref,
    send_ref, recv_ref, tile_sem, send_sem, recv_sem,
):
    src = lax.axis_index("src")
    reg = lax.axis_index("reg")
    me = src * regs + reg
    count = tiles_ref.shape[0]
    width = tiles_ref.shape[2]
    per_chunk = count // chunks
    groups = count // GROUP
    rows = n * stride
    row_blocks = rays_ref.shape[0]

    def tile_copy(c):
        part = pl.ds(c * per_chunk, per_chunk)
        return pltpu.make_async_copy(tiles_hbm.at[part], tiles_ref.at[part], tile_sem.at[c])

    for c in range(chunks):
        tile_copy(c).start()

    barrier = pltpu.get_barrier_semaphore()

    @pl.loop(1, n)
    def _(k):
        d = lax.rem(me + k, n)
        pl.semaphore_signal(
            barrier, inc=1, device_id=(d // regs, lax.rem(d, regs)), device_id_type=MESH
        )

    def hot(a, b):
        return jnp.where(a == b, 1.0, 0.0).astype(BF16)

    iota = functools.partial(lax.broadcasted_iota, jnp.int32)
    live = iota((1, count), 1) < count_ref[0]
    slots = slots_ref[...]
    slots = jnp.where(live, slots // cap * stride + lax.rem(slots, cap), -1)
    one_slot = hot(iota((rows, count), 0), slots)
    one_ray = hot(iota((row_blocks, count), 0), jnp.where(live, rows_ref[...], -1))
    slot_hot[...] = one_slot
    slot_hot_t[...] = one_slot.T
    ray_hot[...] = one_ray
    ray_hot_t[...] = one_ray.T
    wanted = wanted_ref[...].astype(F32)
    row_place = lax.rem(iota((1, rows), 1), stride)
    col_place = lax.rem(iota((rows, 1), 0), stride)
    peers_t = jnp.where(iota((n, rows), 0) == iota((n, rows), 1) // stride, 1.0, 0.0)
    peers = jnp.where(iota((rows, n), 1) == iota((rows, n), 0) // stride, 1.0, 0.0)
    req_row = jnp.where(row_place < cap, 0.0, -1.0)
    req_col = jnp.where(col_place < cap, 0.0, -1.0)
    for k in range(cap):
        asked = wanted[k : k + 1, :]
        req_col += jnp.where(col_place == k, jnp.sum(peers * asked, axis=1, keepdims=True), 0.0)
        picked = jnp.dot(
            jnp.broadcast_to(asked, (8, n)), peers_t, preferred_element_type=F32,
            precision=lax.Precision.HIGHEST,
        )[:1]
        req_row += jnp.where(row_place == k, picked, 0.0)
    same = (req_col == req_row) & (req_col >= 0.0)
    same_ref[...] = jnp.where(same, 1.0, 0.0).astype(BF16)
    lower = jnp.where(same & (iota((rows, rows), 1) < iota((rows, rows), 0)), 1.0, 0.0)
    upper = jnp.where(same & (iota((rows, rows), 0) < iota((rows, rows), 1)), 1.0, 0.0)
    first_col = jnp.where(jnp.sum(lower, axis=1, keepdims=True) == 0.0, 1.0, 0.0)
    first_row = jnp.where(jnp.sum(upper, axis=0, keepdims=True) == 0.0, 1.0, 0.0)
    place = lax.rem(iota((rows, width), 0), stride)
    is_high = place == cap
    is_low = place == cap + 1
    is_sum = is_high | is_low

    def packed(value, squares):
        high = squares.astype(BF16).astype(F32)
        value = jnp.where(is_high, high, value)
        return jnp.where(is_low, squares - high, value).astype(BF16)


    spot = lax.rem(iota((GROUP, width), 0), HALF)
    masks = [jnp.where(spot == b, 1.0, 0.0).astype(BF16) for b in range(HALF)]

    def spread(g):
        base = pl.multiple_of(g * GROUP, GROUP)
        left = left_ref[pl.ds(base, GROUP), :]
        return base, jnp.concatenate([left * m for m in masks], axis=1)

    def keep(base, out):
        mid_ref[pl.ds(base, HALF), :] = out[:HALF, :width]
        mid_ref[pl.ds(pl.multiple_of(base + HALF, HALF), HALF), :] = out[HALF:, width:]

    def group(source, g):
        base, left = spread(g)
        a = source[pl.ds(base, HALF)].reshape(HALF * width, width)
        b = source[pl.ds(base + HALF, HALF)].reshape(HALF * width, width)
        right = jnp.concatenate([a, b], axis=1)
        keep(base, jnp.dot(left, right, preferred_element_type=F32))

    upper_half = me >= n // 2
    skip = jnp.where(upper_half, me, n - 1 - me)

    def exchange(phase, value):
        send_ref[phase] = value.reshape(n, stride, width)

        @pl.loop(0, n - 1)
        def _(j):
            j = j + jnp.where(j >= skip, 1, 0)
            d = jnp.where(upper_half, j, n - 1 - j)
            pltpu.make_async_remote_copy(
                src_ref=send_ref.at[phase, d],
                dst_ref=recv_ref.at[phase, me],
                send_sem=send_sem.at[phase],
                recv_sem=recv_sem.at[phase],
                device_id=(d // regs, lax.rem(d, regs)),
                device_id_type=MESH,
            ).start()

        recv_ref[phase, me] = send_ref[phase, me]
        others = pl.ds(0, n - 1)
        pltpu.make_async_copy(
            recv_ref.at[phase, others], recv_ref.at[phase, others], recv_sem.at[phase]
        ).wait()
        got = recv_ref[phase].reshape(rows, width)
        return got, jnp.sum(
            jnp.where(is_sum, got.astype(F32), 0.0), keepdims=True
        )

    uraw = rays_ref[...]
    u = None
    v = w = update = jnp.zeros((rows, width), F32)
    alpha = phibar = rhobar = None
    fetched = None
    for step in range(ITERS + 1):
        if step > 0:
            left_ref[...] = jnp.dot(
                slot_hot_t[...], fetched, preferred_element_type=F32
            ).astype(BF16)

            @pl.loop(0, groups, unroll=2)
            def _(g):
                group(turned_ref, g)

            uraw = one_hot_dot(ray_hot[...], mid_ref[...]) / alpha - alpha * u
        left_ref[...] = jnp.dot(
            ray_hot_t[...], uraw.astype(BF16), preferred_element_type=F32
        ).astype(BF16)
        if step == 0:
            per = groups // chunks

            @pl.loop(0, chunks)
            def _(c):
                tile_copy(c).wait()
                for i in range(per):
                    group(tiles_ref, c * per + i)

                for i in range(per_chunk):
                    t = c * per_chunk + i
                    turned_ref[t] = tiles_ref[t].T
        else:

            @pl.loop(0, groups, unroll=2)
            def _(g):
                group(tiles_ref, g)

        sums = one_hot_dot(slot_hot[...], mid_ref[...])
        squares = jnp.sum(uraw * uraw, axis=0, keepdims=True)
        if step == 0:
            pl.semaphore_wait(barrier, n - 1)
        got, uu = exchange(2 * step, packed(sums, squares))
        beta = jnp.sqrt(uu)
        u = uraw / beta
        vraw = jnp.dot(same_ref[...], got, preferred_element_type=F32) / beta
        if step > 0:
            vraw = vraw - beta * v
        squares = jnp.sum(vraw * vraw * first_col, axis=0, keepdims=True)
        fetched, vv = exchange(2 * step + 1, packed(vraw, squares))
        alpha = jnp.sqrt(vv)
        v = jnp.where(place < cap, vraw, 0.0) / alpha
        if step == 0:
            w = v
            phibar = beta
            rhobar = alpha
        else:
            rhobar1 = jnp.sqrt(rhobar * rhobar + damping * damping)
            phibar = rhobar / rhobar1 * phibar
            rho = jnp.sqrt(rhobar1 * rhobar1 + beta * beta)
            cosine = rhobar1 / rho
            sine = beta / rho
            theta = sine * alpha
            rhobar = -cosine * alpha
            phi = cosine * phibar
            phibar = sine * phibar
            update = update + phi / rho * w
            w = v - theta / rho * w
    blocks = sol_ref.shape[0]
    out_hot = jnp.where(
        iota((blocks, rows), 0).astype(F32) == req_row, first_row, 0.0
    ).astype(BF16)
    scale = float(blocks * width * n) ** 0.5
    sol_ref[...] = one_hot_dot(out_hot, update, 3)
    right_ref[...] = one_hot_dot(out_hot, v * scale, 3)
    for phase in range(2 * (ITERS + 1)):
        others = pl.ds(0, n - 1)
        pltpu.make_async_copy(
            send_ref.at[phase, others], send_ref.at[phase, others], send_sem.at[phase]
        ).wait()


def per_device(n, regs, tiles, rays, tile_rows, tile_slots, tile_count, wanted):
    count, width = tiles.shape[0], tiles.shape[2]
    cap = wanted.shape[2]
    stride = 4
    while stride < cap + 2:
        stride *= 2
    rows = n * stride
    chunks = 16
    phases = 2 * (ITERS + 1)
    row_blocks = rays.shape[0]
    vmem = pl.BlockSpec(memory_space=pltpu.VMEM)
    out = jax.ShapeDtypeStruct((BLK_DEV, width), F32)
    return pl.pallas_call(
        functools.partial(kernel, n, regs, stride, cap, chunks),
        out_shape=(out, out),
        in_specs=[
            pl.BlockSpec(memory_space=pltpu.SMEM),
            pl.BlockSpec(memory_space=pl.ANY),
        ]
        + [vmem] * 4,
        out_specs=(vmem, vmem),
        scratch_shapes=[
            pltpu.VMEM(tiles.shape, BF16),
            pltpu.VMEM(tiles.shape, BF16),
            pltpu.VMEM((count, width), BF16),
            pltpu.VMEM((count, width), F32),
            pltpu.VMEM((rows, count), BF16),
            pltpu.VMEM((count, rows), BF16),
            pltpu.VMEM((row_blocks, count), BF16),
            pltpu.VMEM((count, row_blocks), BF16),
            pltpu.VMEM((rows, rows), BF16),
            pltpu.VMEM((phases, n, stride, width), BF16),
            pltpu.VMEM((phases, n, stride, width), BF16),
            pltpu.SemaphoreType.DMA((chunks,)),
            pltpu.SemaphoreType.DMA((phases,)),
            pltpu.SemaphoreType.DMA((phases,)),
        ],
        compiler_params=pltpu.CompilerParams(
            collective_id=0, has_side_effects=True, vmem_limit_bytes=56 * 1024 * 1024
        ),
    )(
        tile_count,
        tiles,
        rays,
        tile_rows[None, :],
        tile_slots[None, :],
        wanted[0].T,
    )


def solution(mesh):
    both = ("src", "reg")
    in_specs = (
        P(both, None, None),
        P(both, None),
        P(both),
        P(both),
        P(both),
        P(both, None, None),
    )
    out_specs = (P(both, None), P(both, None))
    n = mesh.shape["src"] * mesh.shape["reg"]
    return jax.shard_map(
        functools.partial(per_device, n, mesh.shape["reg"]),
        mesh=mesh,
        in_specs=in_specs,
        out_specs=out_specs,
        check_vma=False,
    )
```
